1024 devices in a mesh: gx: 8 (over y), gy: 8 (over x, core), gz: 16 (over z).
Axes of the slice: x: 4, y: 8, z: 16, core: 2. Of those that a mesh axis runs over, the one named last changes fastest.
Arguments:
- residual_in: float32 [8, 16, 128, 512], P('gx', 'gy', 'gz'), may hold values from -6 to 6
- geometry: float32 [3, 8, 16, 128], P(None, 'gx', 'gy', 'gz'), may hold values from 0.5 to 2
- eig_top: float32 [2], replicated, may hold values from 1.5 to 2.5
- coarse_rows: float32 [8, 24, 128, 11, 128], P('gx', 'gy', 'gz'), may hold values from -0.21875 to 0.21875
- block_ids: int32 [8, 8, 16, 11], P('gx', 'gy', 'gz'), may hold values from 0 to 2047, as said below
Outputs:
- correction: float32 [8, 16, 128, 512], P('gx', 'gy', 'gz')
The draws below stay inside these ranges and needn't reach their ends.
Inputs may be any that keep to these rules, and one draw needn't show every extreme that they name: `block_ids`: the 11 ids of one row block are distinct.
All inputs are finite; a program needn't handle non-finite values.
Results may differ from the reference program's by a relative error of at most 0.00018.
Values sent between devices are 32-bit elements; how exact they have to be, the bound alone decides.
A program may use at most 64 MiB of HBM per device.

```python
import math
import jax
import jax.numpy as jnp
import numpy as np
from jax import lax

CX = 1
CY = 2
CZ = 8
NF = 8
NM = 4
NC = 2
BW = 128
NB = 11
EXT = 8
EYT = 16
EZT = 128
VY = 24
N_GX = 8
N_GY = 8
N_GZ = 16
DEVICES = 1024


def draw_block_ids(key, part):
    leaf_key = jax.random.fold_in(key, 17)
    label_key = jax.random.fold_in(key, 29)
    leaves = jax.random.permutation(leaf_key, DEVICES).astype(jnp.int32).reshape(N_GX, N_GY, N_GZ, 1)
    levels = jnp.arange(1, NB, dtype=jnp.int32).reshape(1, 1, 1, NB - 1)
    shared = DEVICES - 1 + jnp.right_shift(DEVICES + leaves, levels)
    layout = jnp.concatenate([leaves, jnp.broadcast_to(shared, (N_GX, N_GY, N_GZ, NB - 1))], axis=3)
    labels = jax.random.permutation(label_key, 2 * DEVICES).astype(jnp.int32)
    return labels[layout]


def level_of(rng, dims, split, low, largest):
    def one(dim, blocks):
        steps = jax.random.uniform(jax.random.fold_in(jax.random.fold_in(rng, 6), dim), (blocks,), jnp.float32, low / len(split), largest / len(split))
        return jnp.repeat(jnp.exp(steps), dims[dim] // blocks).reshape((-1,) + (1,) * (len(dims) - dim - 1))

    factor_of = one(*split[0])
    for cut in split[1:]:
        factor_of = factor_of * one(*cut)
    return factor_of


def noise(own_key, shape, scale, most, shards=(), kind=jnp.bfloat16):
    values = scale * jax.random.normal(own_key, shape, jnp.float32)
    if shards:
        values = values * level_of(own_key, shape, shards, -0.22, 0.18)
    return jnp.clip(values, -most, most).astype(kind)


def setup_inputs(seed: int = 0) -> dict:
    streams_of = jax.random.split(jax.random.key(seed), 6)
    residual_in = noise(streams_of[0], (EXT, EYT, EZT, NF ** 3), 1.0, 6.0, ((0, 8), (1, 8), (2, 16)), jnp.float32)
    geometry = jnp.clip(jnp.exp(math.log(2.0) - 1.3862944 * jax.random.uniform(streams_of[1], (3, EXT, EYT, EZT), jnp.float32) ** level_of(streams_of[1], (3, EXT, EYT, EZT), ((1, 8), (2, 8), (3, 16)), -0.2, 0.2)), 0.5, 2.0)
    eig_top = jnp.clip(jax.random.uniform(streams_of[2], (2,), jnp.float32, 1.5, 2.5), 1.5, 2.5)
    coarse_rows = noise(streams_of[3], (EXT, VY, EZT, NB, BW), (0.7 * (2 * BW * CX * (CY + 1) * CZ * DEVICES) ** -0.25), 0.21875, ((0, 8), (1, 8), (2, 16)), jnp.float32)
    block_ids = draw_block_ids(jax.random.fold_in(streams_of[5], 71), 0)
    return dict(residual_in=residual_in, geometry=geometry, eig_top=eig_top, coarse_rows=coarse_rows, block_ids=block_ids)


FULL_PRECISION = lax.Precision.HIGHEST


def legendre_pair(point, degree):
    previous = 1.0
    current = point
    for order in range(1, degree):
        following = ((2 * order + 1) * point * current - order * previous) / (order + 1)
        previous = current
        current = following
    return current, previous


def gll_tables(points):
    degree = points - 1
    node_list = []
    for index in range(points):
        guess = -math.cos(math.pi * index / degree)
        for sweep in range(100):
            high_val, low_val = legendre_pair(guess, degree)
            guess = guess - (guess * high_val - low_val) / (points * high_val)
        node_list.append(guess)
    node_list[0] = -1.0
    node_list[degree] = 1.0
    node_pos = np.array(node_list)
    at_nodes = np.array([legendre_pair(value, degree)[0] for value in node_list])
    weights = 2.0 / (degree * (degree + 1) * at_nodes ** 2)
    derivative = np.zeros((points, points))
    for row_pos in range(points):
        for col_pos in range(points):
            if row_pos != col_pos:
                derivative[row_pos, col_pos] = at_nodes[row_pos] / (at_nodes[col_pos] * (node_pos[row_pos] - node_pos[col_pos]))
    derivative[0, 0] = -degree * (degree + 1) / 4.0
    derivative[degree, degree] = degree * (degree + 1) / 4.0
    stiffness = derivative.T @ (weights[:, None] * derivative)
    return node_pos, weights, stiffness


def interp_table(fine_pts, coarse_pts):
    fine_nodes = gll_tables(fine_pts)[0]
    coarse_nodes = gll_tables(coarse_pts)[0]
    lagrange = np.ones((fine_pts, coarse_pts))
    for col_pos in range(coarse_pts):
        for other_pos in range(coarse_pts):
            if other_pos != col_pos:
                lagrange[:, col_pos] *= (fine_nodes - coarse_nodes[other_pos]) / (coarse_nodes[col_pos] - coarse_nodes[other_pos])
    return lagrange


def level_tables(points):
    node_pos, weights, stiffness = gll_tables(points)
    return jnp.asarray(weights, jnp.float32), jnp.asarray(stiffness, jnp.float32)


def local_apply(nodal, coeffs, weights, stiffness):
    plane_w = weights[:, None] * weights[None, :]
    term_x = jnp.einsum('ia,...abc->...ibc', stiffness, nodal, precision=FULL_PRECISION) * plane_w
    term_y = jnp.einsum('jb,...abc->...ajc', stiffness, nodal, precision=FULL_PRECISION) * plane_w[:, None, :]
    term_z = jnp.einsum('kc,...abc->...abk', stiffness, nodal, precision=FULL_PRECISION) * plane_w[:, :, None]
    return coeffs[0][..., None, None, None] * term_x + coeffs[1][..., None, None, None] * term_y + coeffs[2][..., None, None, None] * term_z


def local_diagonal(coeffs, weights, stiffness):
    stiff_diag = jnp.diag(stiffness)
    part_x = stiff_diag[:, None, None] * weights[None, :, None] * weights[None, None, :]
    part_y = weights[:, None, None] * stiff_diag[None, :, None] * weights[None, None, :]
    part_z = weights[:, None, None] * weights[None, :, None] * stiff_diag[None, None, :]
    return coeffs[0][..., None, None, None] * part_x + coeffs[1][..., None, None, None] * part_y + coeffs[2][..., None, None, None] * part_z


def chebyshev(residual, initial, top_eig, operate, inverse_diag):
    center = 0.55 * top_eig
    spread_eig = 0.45 * top_eig
    sigma_ratio = center / spread_eig
    rho_first = 1.0 / sigma_ratio
    rho_next = 1.0 / (2.0 * sigma_ratio - rho_first)
    if initial is None:
        current = residual
    else:
        current = residual - operate(initial)
    step_one = inverse_diag * current / center
    iterate = step_one if initial is None else initial + step_one
    second_res = residual - operate(iterate)
    step_two = rho_first * rho_next * step_one + (2.0 * rho_next / spread_eig) * (inverse_diag * second_res)
    return iterate + step_two


def prolong(nodal, lagrange):
    nodal = jnp.einsum('ia,...abc->...ibc', lagrange, nodal, precision=FULL_PRECISION)
    nodal = jnp.einsum('jb,...abc->...ajc', lagrange, nodal, precision=FULL_PRECISION)
    return jnp.einsum('kc,...abc->...abk', lagrange, nodal, precision=FULL_PRECISION)


def restrict(nodal, lagrange):
    nodal = jnp.einsum('ia,...ibc->...abc', lagrange, nodal, precision=FULL_PRECISION)
    nodal = jnp.einsum('jb,...ajc->...abc', lagrange, nodal, precision=FULL_PRECISION)
    return jnp.einsum('kc,...abk->...abc', lagrange, nodal, precision=FULL_PRECISION)


def multiplicity(points, elem_y, total_y):
    degree = points - 1
    first_node = (jnp.arange(points) == 0).astype(jnp.float32)
    last_node = (jnp.arange(points) == degree).astype(jnp.float32)
    side_x = 1.0 + first_node + last_node
    low_flag = (elem_y > 0).astype(jnp.float32)
    high_flag = (elem_y < total_y - 1).astype(jnp.float32)
    side_y = 1.0 + low_flag[:, None] * first_node[None, :] + high_flag[:, None] * last_node[None, :]
    return side_x[None, None, None, :, None, None] * side_y[None, :, None, None, :, None] * side_x[None, None, None, None, None, :]


def ref_pass(nodal, direction, periodic):
    dim_count = nodal.ndim
    elem_axis = dim_count - 6 + direction
    point_axis = dim_count - 3 + direction
    degree = nodal.shape[point_axis] - 1
    left_face = jnp.take(nodal, 0, axis=point_axis)
    right_face = jnp.take(nodal, degree, axis=point_axis)
    summed = right_face + jnp.roll(left_face, -1, axis=elem_axis)
    before = jnp.roll(summed, 1, axis=elem_axis)
    if not periodic:
        extent = nodal.shape[elem_axis]
        shape_list = [1] * left_face.ndim
        shape_list[elem_axis] = extent
        where_pos = jnp.arange(extent).reshape(shape_list)
        summed = jnp.where(where_pos == extent - 1, right_face, summed)
        before = jnp.where(where_pos == 0, left_face, before)
    middle = lax.slice_in_dim(nodal, 1, degree, axis=point_axis)
    return jnp.concatenate([jnp.expand_dims(before, point_axis), middle, jnp.expand_dims(summed, point_axis)], axis=point_axis)


def direct_sum(nodal):
    nodal = ref_pass(nodal, 0, True)
    nodal = ref_pass(nodal, 1, False)
    return ref_pass(nodal, 2, True)


def ref_coarse(low_res, coarse_rows, block_ids):
    flat_nodes = low_res.reshape(EXT, EYT, EZT, NC ** 3)
    top_mask = jnp.arange(N_GY) == N_GY - 1
    base_vals = flat_nodes[..., 0].reshape(EXT, N_GY, CY, EZT)
    upper_side = flat_nodes[..., 2].reshape(EXT, N_GY, CY, EZT)[:, :, CY - 1:, :]
    upper_side = jnp.where(top_mask[None, :, None, None], upper_side, 0.0)
    owned_vals = jnp.concatenate([base_vals, upper_side], axis=2).reshape(N_GX, CX, N_GY, CY + 1, N_GZ, CZ)
    row_tiles = coarse_rows.reshape(N_GX, CX, N_GY, CY + 1, N_GZ, CZ, NB, BW)
    contrib = jnp.einsum('aibjck,aibjcknw->abcnw', owned_vals, row_tiles, precision=FULL_PRECISION)
    column = jnp.zeros((2 * DEVICES, BW), jnp.float32).at[block_ids.reshape(-1)].add(contrib.reshape(-1, BW))
    picked = column[block_ids]
    solved = jnp.einsum('aibjcknw,abcnw->aibjck', row_tiles, picked, precision=FULL_PRECISION)
    solved = solved.reshape(EXT, N_GY, CY + 1, EZT)
    top_values = jnp.where(top_mask[None, :, None, None], solved[:, :, CY:, :], 0.0)
    zeros_y = jnp.zeros((EXT, N_GY, CY - 1, EZT), jnp.float32)
    corner_two = jnp.concatenate([zeros_y, top_values], axis=2).reshape(EXT, EYT, EZT)
    corner_zero = solved[:, :, :CY, :].reshape(EXT, EYT, EZT)
    zero_nodes = jnp.zeros_like(corner_zero)
    spread = jnp.stack([corner_zero, zero_nodes, corner_two, zero_nodes, zero_nodes, zero_nodes, zero_nodes, zero_nodes], axis=-1)
    return direct_sum(spread.reshape(EXT, EYT, EZT, NC, NC, NC))


def reference(residual_in, geometry, eig_top, coarse_rows, block_ids):
    fine_w, fine_k = level_tables(NF)
    mid_w, mid_k = level_tables(NM)
    up_mid = jnp.asarray(interp_table(NF, NM), jnp.float32)
    up_low = jnp.asarray(interp_table(NM, NC), jnp.float32)
    elem_y = jnp.arange(EYT)
    source = residual_in.reshape(EXT, EYT, EZT, NF, NF, NF)
    stacked = direct_sum(jnp.stack([source, local_diagonal(geometry, fine_w, fine_k)]))
    fine_res = stacked[0]
    fine_inv = 1.0 / stacked[1]

    def fine_op(nodal):
        return direct_sum(local_apply(nodal, geometry, fine_w, fine_k))

    def mid_op(nodal):
        return direct_sum(local_apply(nodal, geometry, mid_w, mid_k))

    fine_x = chebyshev(fine_res, None, eig_top[0], fine_op, fine_inv)
    fine_left = fine_res - fine_op(fine_x)
    mid_src = restrict(fine_left / multiplicity(NF, elem_y, EYT), up_mid)
    stacked = direct_sum(jnp.stack([mid_src, local_diagonal(geometry, mid_w, mid_k)]))
    mid_res = stacked[0]
    mid_inv = 1.0 / stacked[1]
    mid_x = chebyshev(mid_res, None, eig_top[1], mid_op, mid_inv)
    mid_left = mid_res - mid_op(mid_x)
    low_res = direct_sum(restrict(mid_left / multiplicity(NM, elem_y, EYT), up_low))
    low_u = ref_coarse(low_res, coarse_rows, block_ids)
    mid_x = chebyshev(mid_res, mid_x + prolong(low_u, up_low), eig_top[1], mid_op, mid_inv)
    fine_x = chebyshev(fine_res, fine_x + prolong(mid_x, up_mid), eig_top[0], fine_op, fine_inv)
    return fine_x.reshape(EXT, EYT, EZT, NF ** 3)
```

```python
import functools
import math

import jax
import jax.numpy as jnp
import numpy as np
from jax import lax
from jax.experimental import pallas as pl
from jax.experimental.pallas import tpu as pltpu
from jax.sharding import PartitionSpec as P

NF = 8
NM = 4
NC = 2
NE = 16
ROWS = 64
LANES = 128
SLOTS = 4
OPENING = 3
BLOCKS = 11
PLACE = {8: list(range(8)), 4: [0, 1, 2, 7], 2: [0, 7]}
MESH = pl.DeviceIdType.MESH
HIGHEST = lax.Precision.HIGHEST
AREA = [(dx, dy) for dx in (-1, 0, 1) for dy in (-1, 0, 1)]
FLAT = [d for d in AREA if d != (0, 0)]


def legendre_pair(point, degree):
    previous = 1.0
    current = point
    for order in range(1, degree):
        following = ((2 * order + 1) * point * current - order * previous) / (order + 1)
        previous = current
        current = following
    return (current, previous)


def gll_tables(points):
    degree = points - 1
    node_list = []
    for index in range(points):
        guess = -math.cos(math.pi * index / degree)
        for sweep in range(100):
            high_val, low_val = legendre_pair(guess, degree)
            guess = guess - (guess * high_val - low_val) / (points * high_val)
        node_list.append(guess)
    node_list[0] = -1.0
    node_list[degree] = 1.0
    node_pos = np.array(node_list)
    at_nodes = np.array([legendre_pair(value, degree)[0] for value in node_list])
    weights = 2.0 / (degree * (degree + 1) * at_nodes**2)
    derivative = np.zeros((points, points))
    for row_pos in range(points):
        for col_pos in range(points):
            if row_pos != col_pos:
                derivative[row_pos, col_pos] = at_nodes[row_pos] / (
                    at_nodes[col_pos] * (node_pos[row_pos] - node_pos[col_pos])
                )
    derivative[0, 0] = -degree * (degree + 1) / 4.0
    derivative[degree, degree] = degree * (degree + 1) / 4.0
    stiffness = derivative.T @ (weights[:, None] * derivative)
    return (node_pos, weights, stiffness)


def interp_table(fine_pts, coarse_pts):
    fine_nodes = gll_tables(fine_pts)[0]
    coarse_nodes = gll_tables(coarse_pts)[0]
    lagrange = np.ones((fine_pts, coarse_pts))
    for col_pos in range(coarse_pts):
        for other_pos in range(coarse_pts):
            if other_pos != col_pos:
                lagrange[:, col_pos] *= (fine_nodes - coarse_nodes[other_pos]) / (
                    coarse_nodes[col_pos] - coarse_nodes[other_pos]
                )
    return lagrange


def constant_tables():
    parts = {}
    same = np.eye(NE)
    for points in (NF, NM):
        at = PLACE[points]
        _, short_w, short_k = gll_tables(points)
        short_w = short_w.astype(np.float32).astype(np.float64)
        short_k = short_k.astype(np.float32).astype(np.float64)
        w = np.zeros(8)
        w[at] = short_w
        k = np.zeros((8, 8))
        k[np.ix_(at, at)] = short_k
        kd = np.diag(k)
        parts["left%d" % points] = np.concatenate([np.kron(k, np.diag(w)), np.kron(np.diag(w), k)])
        parts["right%d" % points] = np.kron(same, k.T)
        parts["wab%d" % points] = np.repeat(np.kron(w, w)[:, None], LANES, 1)
        lane_w, lane_k = np.tile(w, NE), np.tile(kd, NE)
        parts["dx%d" % points] = np.kron(kd, w)[:, None] * lane_w
        parts["dy%d" % points] = np.kron(w, kd)[:, None] * lane_w
        parts["dz%d" % points] = np.kron(w, w)[:, None] * lane_k
        parts["lane%d" % points] = np.repeat(lane_w[None], 8, 0)
    for fine, coarse, name in ((NF, NM, "f"), (NM, NC, "c")):
        j = np.zeros((8, 8))
        j[np.ix_(PLACE[fine], PLACE[coarse])] = interp_table(fine, coarse)
        parts["down_left_" + name] = np.kron(j, j).T
        parts["down_right_" + name] = np.kron(same, j)
        parts["up_left_" + name] = np.kron(j, j)
        parts["up_right_" + name] = np.kron(same, j.T)
    parts["spread"] = np.kron(same, np.ones((1, 8)))
    ends = ((0, 64), (64, 0), (63, 127), (127, 63))
    pick = np.zeros((32, LANES))
    for index, pair in enumerate(ends):
        for row, lane in enumerate(pair):
            pick[index * 8 + row, lane] = 1.0
    parts["pick"] = pick
    put = np.zeros((8, LANES))
    for row, lane in enumerate((0, 64, 63, 127)):
        put[row, lane] = 1.0
    parts["put"] = put
    own_low, own_top = np.zeros((24, LANES)), np.zeros((24, LANES))
    for z in range(8):
        own_low[z, z * 8] = 1.0
        own_low[8 + z, 64 + z * 8] = 1.0
        own_top[16 + z, 64 + z * 8] = 1.0
    parts["own_low"], parts["own_top"] = own_low, own_top
    start, rows, where = 0, [], {}
    for name, part in parts.items():
        where[name] = (start, part.shape[0], part.shape[1])
        start += part.shape[0]
        rows.append(np.pad(part, ((0, 0), (0, LANES - part.shape[1]))))
    return np.concatenate(rows).astype(np.float32), where


def dot(a, b):
    return jnp.dot(a, b, precision=HIGHEST, preferred_element_type=jnp.float32)


def dot_nt(a, b):
    return lax.dot_general(
        a, b, (((1,), (1,)), ((), ())), precision=HIGHEST, preferred_element_type=jnp.float32
    )


def dot_tn(a, b):
    return lax.dot_general(
        a, b, (((0,), (0,)), ((), ())), precision=HIGHEST, preferred_element_type=jnp.float32
    )


def kernel(
    sizes, where, src_ref, geo_ref, eig_ref, rows_ref, ids_ref, tab_ref, out_ref,
    work, ysend, zsend, xyrecv, zrecv, zin, idsend, idrecv, csend, crecv, colsend, rsrecv,
    zpsend, zprecv, agsend, agrecv, backsend, backrecv,
    xy_sems, z_sems, id_sems, c_sems, rs_sems, zp_sems, ag_sems, back_sems,
):
    n_x, n_y, n_z = sizes
    me_x, me_y, me_z = lax.axis_index("gx"), lax.axis_index("gy"), lax.axis_index("gz")
    bx, by, bz = n_x // 2, n_y // 4, n_z // 2
    my_place = (me_x % 2) * 8 + (me_y % 4) * 2 + me_z % 2
    my_block = (me_x // 2) * by + me_y // 4

    def table(name):
        start, count, width = where[name]
        return tab_ref[pl.ds(start, count), pl.ds(0, width)]

    def near(dx, dy, dz):
        return ((me_x + dx + n_x) % n_x, (me_y + dy + n_y) % n_y, (me_z + dz + n_z) % n_z)

    def mate(ux, uy, uz):
        px, py, pz = (me_x % 2 + ux) % 2, (me_y % 4 + uy) % 4, (me_z % 2 + uz) % 2
        who = ((me_x // 2) * 2 + px, (me_y // 4) * 4 + py, (me_z // 2) * 2 + pz)
        return who, px * 8 + py * 2 + pz

    def across(tx, ty):
        qx, qy = (me_x // 2 + tx) % bx, (me_y // 4 + ty) % by
        return (qx * 2 + me_x % 2, qy * 4 + me_y % 4, me_z), qx * by + qy

    def along(tz):
        return (me_x, me_y, ((me_z // 2 + tz) % bz) * 2 + me_z % 2)

    mates = [mate(i // 8, i // 2 % 4, i % 2) for i in range(1, 16)]
    crosses = [across(i // by, i % by) for i in range(1, bx * by)]
    lines = [along(i) for i in range(1, bz)]

    barrier = pltpu.get_barrier_semaphore()
    peers = [near(dx, dy, dz) for dx, dy in AREA for dz in (-1, 0, 1) if (dx, dy, dz) != (0, 0, 0)]
    peers += [who for who, _ in mates] + [who for who, _ in crosses] + lines
    for who in peers:
        pl.semaphore_signal(barrier, inc=1, device_id=who, device_id_type=MESH)

    def send(src, dst, sems, who):
        pltpu.make_async_remote_copy(
            src_ref=src, dst_ref=dst, send_sem=sems.at[0], recv_sem=sems.at[1],
            device_id=who, device_id_type=MESH,
        ).start()

    def await_all(ref, sems):
        every = pltpu.make_async_remote_copy(
            src_ref=ref, dst_ref=ref, send_sem=sems.at[0], recv_sem=sems.at[1],
            device_id=near(1, 0, 0), device_id_type=MESH,
        )
        every.wait_recv()
        every.wait_send()

    lane = lax.broadcasted_iota(jnp.int32, (8, LANES), 1)
    row = lax.broadcasted_iota(jnp.int32, (8, LANES), 0)
    low_half = lane < 64
    row64 = lax.broadcasted_iota(jnp.int32, (ROWS, LANES), 0)
    lane64 = lax.broadcasted_iota(jnp.int32, (ROWS, LANES), 1)
    node, elem = lane64 % 8, lane64 // 8 % 8
    join_up = (node == 7) & (elem < 7)
    join_down = (node == 0) & (elem > 0)
    edge_y = ((row64 % 8 == 0) & (lane64 < 64)) | ((row64 % 8 == 7) & (lane64 >= 64))
    has_low = (me_y > 0).astype(jnp.float32)
    has_high = (me_y < n_y - 1).astype(jnp.float32)
    at_top = (me_y == n_y - 1).astype(jnp.float32)

    def roll(value, shift, axis):
        return pltpu.roll(value, shift % value.shape[axis], axis)

    def sum_pack(slot, value):
        field = work.at[slot]
        value = (
            value
            + jnp.where(join_up, roll(value, -1, 1), 0.0)
            + jnp.where(join_down, roll(value, 1, 1), 0.0)
        )
        field[pl.ds(0, ROWS), :] = value
        low = field[pl.ds(0, 8, stride=8), :]
        high = field[pl.ds(7, 8, stride=8), :]
        new_low = low + jnp.where(low_half, 0.0, roll(high, 64, 1))
        new_high = high + jnp.where(low_half, roll(low, 64, 1), 0.0)
        field[pl.ds(0, 8, stride=8), :] = new_low
        field[pl.ds(7, 8, stride=8), :] = new_high
        ysend[slot] = jnp.where(low_half, new_low, new_high)
        ends = dot_nt(table("pick"), field[...])
        for index, (dx, dy) in enumerate(AREA):
            keep = low_half
            if dx:
                keep = keep & (lane // 8 == (0 if dx > 0 else 7))
            if dy:
                keep = keep & (lane % 8 == (0 if dy > 0 else 7)) & (row == (0 if dy > 0 else 1))
            for side in (0, 1):
                variant = 2 * side + (1 if dy else 0)
                tile = ends[variant * 8 : variant * 8 + 8]
                moved = jnp.where(keep, roll(tile, -56 * dx - 7 * dy, 1), 0.0)
                zsend[slot, index * 2 + side] = moved[0:2]

    def sum_send(slot):
        for dx, dy in FLAT:
            there = FLAT.index((-dx, -dy))
            if dy:
                src = ysend.at[slot]
            else:
                src = work.at[slot, pl.ds(56 if dx > 0 else 0, 8), :]
            send(src, xyrecv.at[slot, there], xy_sems.at[slot], near(dx, dy, 0))
        for index, (dx, dy) in enumerate(AREA):
            there = AREA.index((-dx, -dy))
            for side, dz in ((0, -1), (1, 1)):
                send(
                    zsend.at[slot, index * 2 + side],
                    zrecv.at[slot, there * 2 + side],
                    z_sems.at[slot],
                    near(dx, dy, dz),
                )

    def sum_finish(slot):
        await_all(xyrecv.at[slot], xy_sems.at[slot])
        tiles = {d: xyrecv[slot, i] for i, d in enumerate(FLAT)}

        def edge(dy):
            return (
                tiles[(0, dy)]
                + jnp.where(row == 7, roll(tiles[(1, dy)], 7, 0), 0.0)
                + jnp.where(row == 0, roll(tiles[(-1, dy)], 1, 0), 0.0)
            )

        from_y = roll(jnp.where(low_half, edge(1) * has_high, edge(-1) * has_low), 64, 1)
        value = work[slot, pl.ds(0, ROWS), :]
        spread = jnp.broadcast_to(from_y[:, None, :], (8, 8, LANES)).reshape(ROWS, LANES)
        value = value + jnp.where(edge_y, spread, 0.0)
        value = value + jnp.concatenate(
            [tiles[(-1, 0)], jnp.zeros((48, LANES), jnp.float32), tiles[(1, 0)]], axis=0
        )
        await_all(zrecv.at[slot], z_sems.at[slot])
        for side in (0, 1):
            parts = []
            for dy in (-1, 0, 1):
                part = sum(zrecv[slot, AREA.index((dx, dy)) * 2 + side] for dx in (-1, 0, 1))
                parts.append(part if dy == 0 else part * (has_low if dy < 0 else has_high))
            target = 2 * (1 - side)
            zin[pl.ds(target, 2), :] = parts[0] + parts[1] + parts[2]
        return value + dot_tn(zin[...], table("put"))[0:ROWS]

    turn = [OPENING]

    def direct_sum(value):
        slot = turn[0] % SLOTS
        turn[0] += 1
        sum_pack(slot, value)
        sum_send(slot)
        return sum_finish(slot)

    for slot in range(SLOTS):
        work[slot, pl.ds(ROWS, ROWS), :] = jnp.zeros((ROWS, LANES), jnp.float32)
    zin[...] = jnp.zeros_like(zin)
    csend[...] = jnp.zeros_like(csend)

    geo = dot(geo_ref[:, 0, :], table("spread")[0:8]) + dot(geo_ref[:, 1, :], table("spread")[8:16])
    geo = [geo[i : i + 1] for i in range(3)]

    spread16 = dot_tn(src_ref[...], table("spread"))
    deep_row = lax.broadcasted_iota(jnp.int32, (NE * 32, LANES), 0)
    deep_lane = lax.broadcasted_iota(jnp.int32, (NE * 32, LANES), 1)
    same_node = deep_row % 8 == deep_lane % 8
    source = jnp.sum(jnp.where(same_node, spread16, 0.0).reshape(ROWS, 8, LANES), axis=1)

    def diagonal(points):
        return sum(g * table("d%s%d" % (axis, points)) for g, axis in zip(geo, "xyz"))

    scaled = {}
    for points in (NF, NM):
        lane_w = table("lane%d" % points)[0:1]
        scaled[points] = (geo[0] * lane_w, geo[1] * lane_w, geo[2] * table("wab%d" % points))

    def local_apply(value, points):
        in_x, in_y, in_z = scaled[points]
        both = dot(table("left%d" % points), value)
        return (
            in_x * both[0:ROWS]
            + in_y * both[ROWS : 2 * ROWS]
            + in_z * dot(value, table("right%d" % points))
        )

    def move(value, way):
        left, right = way.split("-")
        return dot(dot(table(left), value), table(right))

    def cheb_numbers(index):
        lam = jnp.full((1, LANES), eig_ref[index], jnp.float32)
        center = 0.55 * lam
        spread_eig = 0.45 * lam
        ratio = center / spread_eig
        first = 1.0 / ratio
        following = 1.0 / (2.0 * ratio - first)
        return 1.0 / center, first * following, 2.0 * following / spread_eig

    small_lane = lax.broadcasted_iota(jnp.int32, (2, LANES), 1)
    small_row = lax.broadcasted_iota(jnp.int32, (2, LANES), 0)
    spot = small_row * LANES + small_lane - my_place * 16
    own_ids = jnp.zeros((2, LANES), jnp.float32)
    for k in range(BLOCKS):
        number = jnp.full((2, LANES), ids_ref[k], jnp.int32).astype(jnp.float32) + 1.0
        own_ids = jnp.where(spot == k, number, own_ids)
    idsend[...] = own_ids

    sum_pack(0, source)
    sum_pack(1, diagonal(NF))
    sum_pack(2, diagonal(NM))
    pl.semaphore_wait(barrier, len(peers))
    for slot in range(OPENING):
        sum_send(slot)
    for i, (who, _) in enumerate(mates):
        send(idsend, idrecv.at[i], id_sems, who)
    fine_res = sum_finish(0)
    fine_inv = 1.0 / sum_finish(1)
    mid_diag = sum_finish(2)
    mid_inv = jnp.where(mid_diag > 0.0, 1.0 / jnp.where(mid_diag > 0.0, mid_diag, 1.0), 0.0)

    def chebyshev(residual, initial, numbers, points, inverse):
        by_center, first, second = numbers
        if initial is None:
            current = residual
        else:
            current = residual - direct_sum(local_apply(initial, points))
        step_one = inverse * current * by_center
        iterate = step_one if initial is None else initial + step_one
        left = residual - direct_sum(local_apply(iterate, points))
        return iterate + (first * step_one + second * (inverse * left))

    fine_numbers, mid_numbers = cheb_numbers(0), cheb_numbers(1)
    fine_x = chebyshev(fine_res, None, fine_numbers, NF, fine_inv)
    mid_src = move(source - local_apply(fine_x, NF), "down_left_f-down_right_f")
    mid_res = direct_sum(mid_src)
    mid_x = chebyshev(mid_res, None, mid_numbers, NM, mid_inv)
    low_res = direct_sum(move(mid_src - local_apply(mid_x, NM), "down_left_c-down_right_c"))

    own_low = table("own_low")
    own_top = table("own_top") * at_top
    owned = jnp.sum(own_low * low_res[0:1] + own_top * low_res[7:8], axis=1, keepdims=True)
    owned = jnp.broadcast_to(owned, (24, LANES))
    contrib = jnp.zeros((BLOCKS, LANES), jnp.float32)
    for r in range(24):
        contrib = contrib + owned[r : r + 1] * rows_ref[r]
    csend[pl.ds(0, BLOCKS), :] = contrib
    for who, _ in mates:
        send(csend, crecv.at[my_place], c_sems, who)
    crecv[my_place] = csend[...]

    await_all(idrecv, id_sems)
    all_ids = own_ids
    for i in range(15):
        all_ids = all_ids + idrecv[i]
    wanted = (
        lax.broadcasted_iota(jnp.int32, (LANES, LANES), 0) + my_place * LANES + 1
    ).astype(jnp.float32)
    match_a = (all_ids[0:1] == wanted).astype(jnp.float32)
    match_b = (all_ids[1:2] == wanted).astype(jnp.float32)

    await_all(crecv.at[pl.ds(0, 15)], c_sems)
    part = dot(match_a, crecv[pl.ds(0, 8)].reshape(LANES, LANES)) + dot(
        match_b, crecv[pl.ds(8, 8)].reshape(LANES, LANES)
    )
    peers_xy = bx * by
    height = LANES // peers_xy
    colsend[...] = part.reshape(peers_xy, height, LANES)
    for i, (who, block) in enumerate(crosses):
        send(colsend.at[block], rsrecv.at[i], rs_sems, who)
    piece = colsend[my_block]
    await_all(rsrecv, rs_sems)
    for i in range(peers_xy - 1):
        piece = piece + rsrecv[i]
    zpsend[...] = piece
    for i, who in enumerate(lines):
        send(zpsend, zprecv.at[i], zp_sems, who)
    await_all(zprecv, zp_sems)
    for i in range(bz - 1):
        piece = piece + zprecv[i]
    agsend[...] = piece
    for who, _ in crosses:
        send(agsend, agrecv.at[my_block], ag_sems, who)
    agrecv[my_block] = piece
    await_all(agrecv.at[pl.ds(0, peers_xy - 1)], ag_sems)
    slice_sum = agrecv[...].reshape(LANES, LANES)
    backsend[pl.ds(0, 8)] = dot_tn(match_a, slice_sum).reshape(8, 16, LANES)
    backsend[pl.ds(8, 8)] = dot_tn(match_b, slice_sum).reshape(8, 16, LANES)
    for i, (who, place) in enumerate(mates):
        send(backsend.at[place], backrecv.at[i], back_sems, who)
    picked = backsend[my_place]
    await_all(backrecv, back_sems)
    for i in range(15):
        picked = picked + backrecv[i]

    solved = jnp.sum(rows_ref[...] * picked[None, 0:BLOCKS], axis=1)
    solved = jnp.sum(solved, axis=1, keepdims=True)
    at_low = jnp.sum(own_low * solved, axis=0, keepdims=True)
    at_high = jnp.sum(own_top * solved, axis=0, keepdims=True)
    low_u = direct_sum(
        jnp.where(row64 == 0, at_low, 0.0) + jnp.where(row64 == 7, at_high, 0.0)
    )
    mid_x = chebyshev(mid_res, mid_x + move(low_u, "up_left_c-up_right_c"), mid_numbers, NM, mid_inv)
    fine_x = chebyshev(
        fine_res, fine_x + move(mid_x, "up_left_f-up_right_f"), fine_numbers, NF, fine_inv
    )
    deep = jnp.broadcast_to(fine_x[:, None, :], (ROWS, 8, LANES)).reshape(ROWS * 8, LANES)
    out_ref[...] = dot_nt(table("spread"), jnp.where(same_node, deep, 0.0))


def solution(mesh):
    sizes = (mesh.shape["gx"], mesh.shape["gy"], mesh.shape["gz"])
    values, where = constant_tables()
    peers_xy = (sizes[0] // 2) * (sizes[1] // 4)
    height = LANES // peers_xy
    depth = sizes[2] // 2
    f32 = jnp.float32

    def on_device(residual_in, geometry, eig_top, coarse_rows, block_ids):
        vmem = pl.BlockSpec(memory_space=pltpu.VMEM)
        smem = pl.BlockSpec(memory_space=pltpu.SMEM)
        pair = pltpu.SemaphoreType.DMA((2,))
        out = pl.pallas_call(
            functools.partial(kernel, sizes, where),
            out_shape=jax.ShapeDtypeStruct((NE, NF**3), f32),
            in_specs=[vmem, vmem, smem, vmem, smem, vmem],
            out_specs=vmem,
            scratch_shapes=[
                pltpu.VMEM((SLOTS, 2 * ROWS, LANES), f32),
                pltpu.VMEM((SLOTS, 8, LANES), f32),
                pltpu.VMEM((SLOTS, 18, 2, LANES), f32),
                pltpu.VMEM((SLOTS, 8, 8, LANES), f32),
                pltpu.VMEM((SLOTS, 18, 2, LANES), f32),
                pltpu.VMEM((8, LANES), f32),
                pltpu.VMEM((2, LANES), f32),
                pltpu.VMEM((15, 2, LANES), f32),
                pltpu.VMEM((16, LANES), f32),
                pltpu.VMEM((16, 16, LANES), f32),
                pltpu.VMEM((peers_xy, height, LANES), f32),
                pltpu.VMEM((peers_xy - 1, height, LANES), f32),
                pltpu.VMEM((height, LANES), f32),
                pltpu.VMEM((depth - 1, height, LANES), f32),
                pltpu.VMEM((height, LANES), f32),
                pltpu.VMEM((peers_xy, height, LANES), f32),
                pltpu.VMEM((16, 16, LANES), f32),
                pltpu.VMEM((15, 16, LANES), f32),
                pltpu.SemaphoreType.DMA((SLOTS, 2)),
                pltpu.SemaphoreType.DMA((SLOTS, 2)),
                pair, pair, pair, pair, pair, pair,
            ],
            compiler_params=pltpu.CompilerParams(
                collective_id=0, has_side_effects=True, vmem_limit_bytes=32 * 2**20
            ),
        )(
            residual_in.reshape(NE, NF**3),
            geometry.reshape(3, 2, 8),
            eig_top,
            coarse_rows.reshape(24, BLOCKS, LANES),
            block_ids.reshape(BLOCKS),
            jnp.asarray(values),
        )
        return out.reshape(residual_in.shape)

    grid = P("gx", "gy", "gz", None)
    return jax.shard_map(
        on_device,
        mesh=mesh,
        in_specs=(grid, P(None, "gx", "gy", "gz"), P(), P("gx", "gy", "gz", None, None), grid),
        out_specs=grid,
        check_vma=False,
    )
```

```python
import functools
import math

import jax
import jax.numpy as jnp
import numpy as np
from jax import lax
from jax.experimental import pallas as pl
from jax.experimental.pallas import tpu as pltpu
from jax.sharding import PartitionSpec as P

NF = 8
NM = 4
NC = 2
NE = 16
ROWS = 64
LANES = 128
SLOTS = 4
OPENING = 3
BLOCKS = 11
PLACE = {8: list(range(8)), 4: [0, 1, 2, 7], 2: [0, 7]}
MESH = pl.DeviceIdType.MESH
HIGHEST = lax.Precision.HIGHEST
AREA = [(dx, dy) for dx in (-1, 0, 1) for dy in (-1, 0, 1)]
FLAT = [d for d in AREA if d != (0, 0)]


def legendre_pair(point, degree):
    previous = 1.0
    current = point
    for order in range(1, degree):
        following = ((2 * order + 1) * point * current - order * previous) / (order + 1)
        previous = current
        current = following
    return (current, previous)


def gll_tables(points):
    degree = points - 1
    node_list = []
    for index in range(points):
        guess = -math.cos(math.pi * index / degree)
        for sweep in range(100):
            high_val, low_val = legendre_pair(guess, degree)
            guess = guess - (guess * high_val - low_val) / (points * high_val)
        node_list.append(guess)
    node_list[0] = -1.0
    node_list[degree] = 1.0
    node_pos = np.array(node_list)
    at_nodes = np.array([legendre_pair(value, degree)[0] for value in node_list])
    weights = 2.0 / (degree * (degree + 1) * at_nodes**2)
    derivative = np.zeros((points, points))
    for row_pos in range(points):
        for col_pos in range(points):
            if row_pos != col_pos:
                derivative[row_pos, col_pos] = at_nodes[row_pos] / (
                    at_nodes[col_pos] * (node_pos[row_pos] - node_pos[col_pos])
                )
    derivative[0, 0] = -degree * (degree + 1) / 4.0
    derivative[degree, degree] = degree * (degree + 1) / 4.0
    stiffness = derivative.T @ (weights[:, None] * derivative)
    return (node_pos, weights, stiffness)


def interp_table(fine_pts, coarse_pts):
    fine_nodes = gll_tables(fine_pts)[0]
    coarse_nodes = gll_tables(coarse_pts)[0]
    lagrange = np.ones((fine_pts, coarse_pts))
    for col_pos in range(coarse_pts):
        for other_pos in range(coarse_pts):
            if other_pos != col_pos:
                lagrange[:, col_pos] *= (fine_nodes - coarse_nodes[other_pos]) / (
                    coarse_nodes[col_pos] - coarse_nodes[other_pos]
                )
    return lagrange


def constant_tables():
    parts = {}
    same = np.eye(NE)
    for points in (NF, NM):
        at = PLACE[points]
        _, short_w, short_k = gll_tables(points)
        short_w = short_w.astype(np.float32).astype(np.float64)
        short_k = short_k.astype(np.float32).astype(np.float64)
        w = np.zeros(8)
        w[at] = short_w
        k = np.zeros((8, 8))
        k[np.ix_(at, at)] = short_k
        kd = np.diag(k)
        parts["left%d" % points] = np.concatenate([np.kron(k, np.diag(w)), np.kron(np.diag(w), k)])
        parts["right%d" % points] = np.kron(same, k.T)
        parts["wab%d" % points] = np.repeat(np.kron(w, w)[:, None], LANES, 1)
        lane_w, lane_k = np.tile(w, NE), np.tile(kd, NE)
        parts["dx%d" % points] = np.kron(kd, w)[:, None] * lane_w
        parts["dy%d" % points] = np.kron(w, kd)[:, None] * lane_w
        parts["dz%d" % points] = np.kron(w, w)[:, None] * lane_k
        parts["lane%d" % points] = np.repeat(lane_w[None], 8, 0)
    for fine, coarse, name in ((NF, NM, "f"), (NM, NC, "c")):
        j = np.zeros((8, 8))
        j[np.ix_(PLACE[fine], PLACE[coarse])] = interp_table(fine, coarse)
        parts["down_left_" + name] = np.kron(j, j).T
        parts["down_right_" + name] = np.kron(same, j)
        parts["up_left_" + name] = np.kron(j, j)
        parts["up_right_" + name] = np.kron(same, j.T)
    parts["spread"] = np.kron(same, np.ones((1, 8)))
    ends = ((0, 64), (64, 0), (63, 127), (127, 63))
    pick = np.zeros((32, LANES))
    for index, pair in enumerate(ends):
        for row, lane in enumerate(pair):
            pick[index * 8 + row, lane] = 1.0
    parts["pick"] = pick
    put = np.zeros((8, LANES))
    for row, lane in enumerate((0, 64, 63, 127)):
        put[row, lane] = 1.0
    parts["put"] = put
    own_low, own_top = np.zeros((24, LANES)), np.zeros((24, LANES))
    for z in range(8):
        own_low[z, z * 8] = 1.0
        own_low[8 + z, 64 + z * 8] = 1.0
        own_top[16 + z, 64 + z * 8] = 1.0
    parts["own_low"], parts["own_top"] = own_low, own_top
    start, rows, where = 0, [], {}
    for name, part in parts.items():
        where[name] = (start, part.shape[0], part.shape[1])
        start += part.shape[0]
        rows.append(np.pad(part, ((0, 0), (0, LANES - part.shape[1]))))
    return np.concatenate(rows).astype(np.float32), where


def dot(a, b):
    return jnp.dot(a, b, precision=HIGHEST, preferred_element_type=jnp.float32)


def split(value):
    high = value.astype(jnp.bfloat16)
    return high, (value - high.astype(jnp.float32)).astype(jnp.bfloat16)


def dot3(a, b):
    (a_high, a_low), (b_high, b_low) = split(a), split(b)

    def one(left, right):
        return jnp.dot(left, right, preferred_element_type=jnp.float32)

    return one(a_high, b_high) + (one(a_high, b_low) + one(a_low, b_high))


def dot_nt(a, b):
    return lax.dot_general(
        a, b, (((1,), (1,)), ((), ())), precision=HIGHEST, preferred_element_type=jnp.float32
    )


def dot_tn(a, b):
    return lax.dot_general(
        a, b, (((0,), (0,)), ((), ())), precision=HIGHEST, preferred_element_type=jnp.float32
    )


def kernel(
    sizes, where, src_far, geo_ref, eig_ref, rows_far, ids_ref, tab_far, out_ref,
    src_ref, rows_ref, tab_ref, near_sems, work, ysend, zsend, xyrecv, zrecv, zin, idsend, idrecv, csend, crecv, colsend, rsrecv,
    zpsend, zprecv, agsend, agrecv, backsend, backrecv,
    xy_sems, z_sems, id_sems, c_sems, rs_sems, zp_sems, ag_sems, back_sems,
):
    n_x, n_y, n_z = sizes
    fetch_tab = pltpu.make_async_copy(tab_far, tab_ref, near_sems.at[0])
    fetch_rows = pltpu.make_async_copy(rows_far, rows_ref, near_sems.at[1])
    fetch_src = pltpu.make_async_copy(src_far, src_ref, near_sems.at[2])
    fetch_src.start()
    fetch_tab.start()
    fetch_rows.start()
    crecv[...] = jnp.zeros_like(crecv)
    me_x, me_y, me_z = lax.axis_index("gx"), lax.axis_index("gy"), lax.axis_index("gz")
    bx, by, bz = n_x // 2, n_y // 4, n_z // 2
    my_place = (me_x % 2) * 8 + (me_y % 4) * 2 + me_z % 2
    my_block = (me_x // 2) * by + me_y // 4

    def table(name):
        start, count, width = where[name]
        return tab_ref[pl.ds(start, count), pl.ds(0, width)]

    def near(dx, dy, dz):
        return ((me_x + dx + n_x) % n_x, (me_y + dy + n_y) % n_y, (me_z + dz + n_z) % n_z)

    def mate(ux, uy, uz):
        px, py, pz = (me_x % 2 + ux) % 2, (me_y % 4 + uy) % 4, (me_z % 2 + uz) % 2
        who = ((me_x // 2) * 2 + px, (me_y // 4) * 4 + py, (me_z // 2) * 2 + pz)
        return who, px * 8 + py * 2 + pz

    def across(tx, ty):
        qx, qy = (me_x // 2 + tx) % bx, (me_y // 4 + ty) % by
        return (qx * 2 + me_x % 2, qy * 4 + me_y % 4, me_z), qx * by + qy

    def along(tz):
        return (me_x, me_y, ((me_z // 2 + tz) % bz) * 2 + me_z % 2)

    mates = [mate(i // 8, i // 2 % 4, i % 2) for i in range(1, 16)]
    crosses = [across(i // by, i % by) for i in range(1, bx * by)]
    lines = [along(i) for i in range(1, bz)]

    barrier = pltpu.get_barrier_semaphore()
    peers = [near(dx, dy, dz) for dx, dy in AREA for dz in (-1, 0, 1) if (dx, dy, dz) != (0, 0, 0)]
    peers += [who for who, _ in mates] + [who for who, _ in crosses] + lines
    for who in peers:
        pl.semaphore_signal(barrier, inc=1, device_id=who, device_id_type=MESH)

    def send(src, dst, sems, who):
        pltpu.make_async_remote_copy(
            src_ref=src, dst_ref=dst, send_sem=sems.at[0], recv_sem=sems.at[1],
            device_id=who, device_id_type=MESH,
        ).start()

    def await_all(ref, sems):
        every = pltpu.make_async_remote_copy(
            src_ref=ref, dst_ref=ref, send_sem=sems.at[0], recv_sem=sems.at[1],
            device_id=near(1, 0, 0), device_id_type=MESH,
        )
        every.wait_recv()
        every.wait_send()

    lane = lax.broadcasted_iota(jnp.int32, (8, LANES), 1)
    row = lax.broadcasted_iota(jnp.int32, (8, LANES), 0)
    low_half = lane < 64
    row64 = lax.broadcasted_iota(jnp.int32, (ROWS, LANES), 0)
    lane64 = lax.broadcasted_iota(jnp.int32, (ROWS, LANES), 1)
    node, elem = lane64 % 8, lane64 // 8 % 8
    join_up = (node == 7) & (elem < 7)
    join_down = (node == 0) & (elem > 0)
    edge_y = ((row64 % 8 == 0) & (lane64 < 64)) | ((row64 % 8 == 7) & (lane64 >= 64))
    has_low = (me_y > 0).astype(jnp.float32)
    has_high = (me_y < n_y - 1).astype(jnp.float32)
    at_top = (me_y == n_y - 1).astype(jnp.float32)

    def roll(value, shift, axis):
        return pltpu.roll(value, shift % value.shape[axis], axis)

    def sum_pack(slot, value):
        field = work.at[slot]
        value = (
            value
            + jnp.where(join_up, roll(value, -1, 1), 0.0)
            + jnp.where(join_down, roll(value, 1, 1), 0.0)
        )
        field[pl.ds(0, ROWS), :] = value
        low = field[pl.ds(0, 8, stride=8), :]
        high = field[pl.ds(7, 8, stride=8), :]
        new_low = low + jnp.where(low_half, 0.0, roll(high, 64, 1))
        new_high = high + jnp.where(low_half, roll(low, 64, 1), 0.0)
        field[pl.ds(0, 8, stride=8), :] = new_low
        field[pl.ds(7, 8, stride=8), :] = new_high
        ysend[slot] = jnp.where(low_half, new_low, new_high)
        ends = dot_nt(table("pick"), field[...])
        for index, (dx, dy) in enumerate(AREA):
            keep = low_half
            if dx:
                keep = keep & (lane // 8 == (0 if dx > 0 else 7))
            if dy:
                keep = keep & (lane % 8 == (0 if dy > 0 else 7)) & (row == (0 if dy > 0 else 1))
            for side in (0, 1):
                variant = 2 * side + (1 if dy else 0)
                tile = ends[variant * 8 : variant * 8 + 8]
                moved = jnp.where(keep, roll(tile, -56 * dx - 7 * dy, 1), 0.0)
                zsend[slot, index * 2 + side] = moved[0:2]

    def sum_send(slot, fields=1):
        span = pl.ds(slot, fields)
        order = [(dx, dy, dz) for dx, dy in AREA for dz in (-1, 0, 1) if (dx, dy, dz) != (0, 0, 0)]
        for dx, dy, dz in sorted(order, key=lambda d: -sum(map(abs, d))):
            if dz:
                side = 0 if dz < 0 else 1
                src = zsend.at[span, AREA.index((dx, dy)) * 2 + side]
                dst = zrecv.at[span, AREA.index((-dx, -dy)) * 2 + side]
                send(src, dst, z_sems.at[slot], near(dx, dy, dz))
            else:
                if dy:
                    src = ysend.at[span]
                else:
                    src = work.at[span, pl.ds(56 if dx > 0 else 0, 8), :]
                dst = xyrecv.at[span, FLAT.index((-dx, -dy))]
                send(src, dst, xy_sems.at[slot], near(dx, dy, dz))

    def sum_await(slot, fields=1):
        await_all(xyrecv.at[pl.ds(slot, fields)], xy_sems.at[slot])
        await_all(zrecv.at[pl.ds(slot, fields)], z_sems.at[slot])

    def sum_finish(slot):
        tiles = {d: xyrecv[slot, i] for i, d in enumerate(FLAT)}

        def edge(dy):
            return (
                tiles[(0, dy)]
                + jnp.where(row == 7, roll(tiles[(1, dy)], 7, 0), 0.0)
                + jnp.where(row == 0, roll(tiles[(-1, dy)], 1, 0), 0.0)
            )

        from_y = roll(jnp.where(low_half, edge(1) * has_high, edge(-1) * has_low), 64, 1)
        value = work[slot, pl.ds(0, ROWS), :]
        spread = jnp.broadcast_to(from_y[:, None, :], (8, 8, LANES)).reshape(ROWS, LANES)
        value = value + jnp.where(edge_y, spread, 0.0)
        value = value + jnp.concatenate(
            [tiles[(-1, 0)], jnp.zeros((48, LANES), jnp.float32), tiles[(1, 0)]], axis=0
        )
        for side in (0, 1):
            parts = []
            for dy in (-1, 0, 1):
                part = sum(zrecv[slot, AREA.index((dx, dy)) * 2 + side] for dx in (-1, 0, 1))
                parts.append(part if dy == 0 else part * (has_low if dy < 0 else has_high))
            target = 2 * (1 - side)
            zin[pl.ds(target, 2), :] = parts[0] + parts[1] + parts[2]
        return value + dot_tn(zin[...], table("put"))[0:ROWS]

    turn = [OPENING]

    def direct_sum(value):
        slot = turn[0] % SLOTS
        turn[0] += 1
        sum_pack(slot, value)
        sum_send(slot)
        sum_await(slot)
        return sum_finish(slot)

    fetch_src.wait()
    fetch_tab.wait()
    for slot in range(SLOTS):
        work[slot, pl.ds(ROWS, ROWS), :] = jnp.zeros((ROWS, LANES), jnp.float32)
    zin[...] = jnp.zeros_like(zin)

    geo = dot(geo_ref[:, 0, :], table("spread")[0:8]) + dot(geo_ref[:, 1, :], table("spread")[8:16])
    geo = [geo[i : i + 1] for i in range(3)]

    spread16 = dot_tn(src_ref[...], table("spread"))
    deep_row = lax.broadcasted_iota(jnp.int32, (NE * 32, LANES), 0)
    deep_lane = lax.broadcasted_iota(jnp.int32, (NE * 32, LANES), 1)
    same_node = deep_row % 8 == deep_lane % 8
    source = jnp.sum(jnp.where(same_node, spread16, 0.0).reshape(ROWS, 8, LANES), axis=1)

    def diagonal(points):
        return sum(g * table("d%s%d" % (axis, points)) for g, axis in zip(geo, "xyz"))

    scaled = {}
    for points in (NF, NM):
        lane_w = table("lane%d" % points)[0:1]
        scaled[points] = (geo[0] * lane_w, geo[1] * lane_w, geo[2] * table("wab%d" % points))

    def local_apply(value, points):
        in_x, in_y, in_z = scaled[points]
        both = dot3(table("left%d" % points), value)
        return (
            in_x * both[0:ROWS]
            + in_y * both[ROWS : 2 * ROWS]
            + in_z * dot3(value, table("right%d" % points))
        )

    def move(value, way):
        left, right = way.split("-")
        return dot3(dot3(table(left), value), table(right))

    def cheb_numbers(index):
        lam = jnp.full((1, LANES), eig_ref[index], jnp.float32)
        center = 0.55 * lam
        spread_eig = 0.45 * lam
        ratio = center / spread_eig
        first = 1.0 / ratio
        following = 1.0 / (2.0 * ratio - first)
        return 1.0 / center, first * following, 2.0 * following / spread_eig

    small_lane = lax.broadcasted_iota(jnp.int32, (2, LANES), 1)
    small_row = lax.broadcasted_iota(jnp.int32, (2, LANES), 0)
    spot = small_row * LANES + small_lane - my_place * 16
    own_ids = jnp.zeros((2, LANES), jnp.float32)
    for k in range(BLOCKS):
        number = jnp.full((2, LANES), ids_ref[k], jnp.int32).astype(jnp.float32) + 1.0
        own_ids = jnp.where(spot == k, number, own_ids)
    idsend[...] = own_ids

    sum_pack(0, source)
    sum_pack(1, diagonal(NF))
    sum_pack(2, diagonal(NM))
    pl.semaphore_wait(barrier, len(peers))
    sum_send(0, OPENING)
    for i, (who, _) in enumerate(mates):
        send(idsend, idrecv.at[i], id_sems, who)
    sum_await(0, OPENING)
    fine_res = sum_finish(0)
    fine_inv = 1.0 / sum_finish(1)
    mid_diag = sum_finish(2)
    mid_inv = jnp.where(mid_diag > 0.0, 1.0 / jnp.where(mid_diag > 0.0, mid_diag, 1.0), 0.0)

    def chebyshev(residual, initial, numbers, points, inverse):
        by_center, first, second = numbers
        if initial is None:
            current = residual
        else:
            current = residual - direct_sum(local_apply(initial, points))
        step_one = inverse * current * by_center
        iterate = step_one if initial is None else initial + step_one
        left = residual - direct_sum(local_apply(iterate, points))
        return iterate + (first * step_one + second * (inverse * left))

    fine_numbers, mid_numbers = cheb_numbers(0), cheb_numbers(1)
    fine_x = chebyshev(fine_res, None, fine_numbers, NF, fine_inv)
    mid_src = move(source - local_apply(fine_x, NF), "down_left_f-down_right_f")
    mid_res = direct_sum(mid_src)
    mid_x = chebyshev(mid_res, None, mid_numbers, NM, mid_inv)
    low_res = direct_sum(move(mid_src - local_apply(mid_x, NM), "down_left_c-down_right_c"))

    own_low = table("own_low")
    own_top = table("own_top") * at_top
    owned = jnp.sum(own_low * low_res[0:1] + own_top * low_res[7:8], axis=1, keepdims=True)
    owned = jnp.broadcast_to(owned, (24, LANES)).reshape(3, 8, LANES)
    fetch_rows.wait()
    contrib = (
        owned[0:1] * rows_ref[0] + owned[1:2] * rows_ref[1] + owned[2:3] * rows_ref[2]
    )
    contrib = jnp.sum(contrib, axis=1)
    csend[...] = contrib
    for who, _ in mates:
        send(csend, crecv.at[my_place, pl.ds(0, BLOCKS)], c_sems, who)
    crecv[my_place, pl.ds(0, BLOCKS)] = contrib

    await_all(idrecv, id_sems)
    all_ids = own_ids
    for i in range(15):
        all_ids = all_ids + idrecv[i]
    wanted = (
        lax.broadcasted_iota(jnp.int32, (LANES, LANES), 0) + my_place * LANES + 1
    ).astype(jnp.float32)
    match_a = (all_ids[0:1] == wanted).astype(jnp.float32)
    match_b = (all_ids[1:2] == wanted).astype(jnp.float32)

    await_all(crecv.at[pl.ds(0, 15), pl.ds(0, BLOCKS)], c_sems)
    part = dot(match_a, crecv[pl.ds(0, 8)].reshape(LANES, LANES)) + dot(
        match_b, crecv[pl.ds(8, 8)].reshape(LANES, LANES)
    )
    peers_xy = bx * by
    height = LANES // peers_xy
    colsend[...] = part.reshape(peers_xy, height, LANES)
    for i, (who, block) in enumerate(crosses):
        send(colsend.at[block], rsrecv.at[i], rs_sems, who)
    piece = colsend[my_block]
    await_all(rsrecv, rs_sems)
    for i in range(peers_xy - 1):
        piece = piece + rsrecv[i]
    zpsend[...] = piece
    for i, who in enumerate(lines):
        send(zpsend, zprecv.at[i], zp_sems, who)
    await_all(zprecv, zp_sems)
    for i in range(bz - 1):
        piece = piece + zprecv[i]
    agsend[...] = piece
    for who, _ in crosses:
        send(agsend, agrecv.at[my_block], ag_sems, who)
    agrecv[my_block] = piece
    await_all(agrecv.at[pl.ds(0, peers_xy - 1)], ag_sems)
    slice_sum = agrecv[...].reshape(LANES, LANES)
    backsend[pl.ds(0, 8)] = dot_tn(match_a, slice_sum).reshape(8, 16, LANES)
    backsend[pl.ds(8, 8)] = dot_tn(match_b, slice_sum).reshape(8, 16, LANES)
    for i, (who, place) in enumerate(mates):
        send(backsend.at[place, pl.ds(0, BLOCKS)], backrecv.at[i], back_sems, who)
    picked = backsend[my_place, pl.ds(0, BLOCKS)]
    await_all(backrecv, back_sems)
    for i in range(15):
        picked = picked + backrecv[i]

    solved = jnp.concatenate(
        [sum(rows_ref[j, k] * picked[k : k + 1] for k in range(BLOCKS)) for j in range(3)], axis=0
    )
    solved = jnp.sum(solved, axis=1, keepdims=True)
    at_low = jnp.sum(own_low * solved, axis=0, keepdims=True)
    at_high = jnp.sum(own_top * solved, axis=0, keepdims=True)
    low_u = direct_sum(
        jnp.where(row64 == 0, at_low, 0.0) + jnp.where(row64 == 7, at_high, 0.0)
    )
    mid_x = chebyshev(mid_res, mid_x + move(low_u, "up_left_c-up_right_c"), mid_numbers, NM, mid_inv)
    fine_x = chebyshev(
        fine_res, fine_x + move(mid_x, "up_left_f-up_right_f"), fine_numbers, NF, fine_inv
    )
    deep = jnp.broadcast_to(fine_x[:, None, :], (ROWS, 8, LANES)).reshape(ROWS * 8, LANES)
    out_ref[...] = dot_nt(table("spread"), jnp.where(same_node, deep, 0.0))


def solution(mesh):
    sizes = (mesh.shape["gx"], mesh.shape["gy"], mesh.shape["gz"])
    values, where = constant_tables()
    peers_xy = (sizes[0] // 2) * (sizes[1] // 4)
    height = LANES // peers_xy
    depth = sizes[2] // 2
    f32 = jnp.float32

    def on_device(residual_in, geometry, eig_top, coarse_rows, block_ids):
        vmem = pl.BlockSpec(memory_space=pltpu.VMEM)
        smem = pl.BlockSpec(memory_space=pltpu.SMEM)
        far = pl.BlockSpec(memory_space=pltpu.HBM)
        pair = pltpu.SemaphoreType.DMA((2,))
        out = pl.pallas_call(
            functools.partial(kernel, sizes, where),
            out_shape=jax.ShapeDtypeStruct((NE, NF**3), f32),
            in_specs=[far, vmem, smem, far, smem, far],
            out_specs=vmem,
            scratch_shapes=[
                pltpu.VMEM((NE, NF**3), f32),
                pltpu.VMEM((3, BLOCKS, 8, LANES), f32),
                pltpu.VMEM(values.shape, f32),
                pltpu.SemaphoreType.DMA((3,)),
                pltpu.VMEM((SLOTS, 2 * ROWS, LANES), f32),
                pltpu.VMEM((SLOTS, 8, LANES), f32),
                pltpu.VMEM((SLOTS, 18, 2, LANES), f32),
                pltpu.VMEM((SLOTS, 8, 8, LANES), f32),
                pltpu.VMEM((SLOTS, 18, 2, LANES), f32),
                pltpu.VMEM((8, LANES), f32),
                pltpu.VMEM((2, LANES), f32),
                pltpu.VMEM((15, 2, LANES), f32),
                pltpu.VMEM((BLOCKS, LANES), f32),
                pltpu.VMEM((16, 16, LANES), f32),
                pltpu.VMEM((peers_xy, height, LANES), f32),
                pltpu.VMEM((peers_xy - 1, height, LANES), f32),
                pltpu.VMEM((height, LANES), f32),
                pltpu.VMEM((depth - 1, height, LANES), f32),
                pltpu.VMEM((height, LANES), f32),
                pltpu.VMEM((peers_xy, height, LANES), f32),
                pltpu.VMEM((16, 16, LANES), f32),
                pltpu.VMEM((15, BLOCKS, LANES), f32),
                pltpu.SemaphoreType.DMA((SLOTS, 2)),
                pltpu.SemaphoreType.DMA((SLOTS, 2)),
                pair, pair, pair, pair, pair, pair,
            ],
            compiler_params=pltpu.CompilerParams(
                collective_id=0, has_side_effects=True
            ),
        )(
            residual_in.reshape(NE, NF**3),
            geometry.reshape(3, 2, 8),
            eig_top,
            jnp.swapaxes(coarse_rows.reshape(3, 8, BLOCKS, LANES), 1, 2),
            block_ids.reshape(BLOCKS),
            jnp.asarray(values),
        )
        return out.reshape(residual_in.shape)

    grid = P("gx", "gy", "gz", None)
    return jax.shard_map(
        on_device,
        mesh=mesh,
        in_specs=(grid, P(None, "gx", "gy", "gz"), P(), P("gx", "gy", "gz", None, None), grid),
        out_specs=grid,
        check_vma=False,
    )
```

```python
import functools
import math

import jax
import jax.numpy as jnp
import numpy as np
from jax import lax
from jax.experimental import pallas as pl
from jax.experimental.pallas import tpu as pltpu
from jax.sharding import PartitionSpec as P

NF = 8
NM = 4
NC = 2
NE = 16
ROWS = 64
LANES = 128
SLOTS = 4
OPENING = 3
BLOCKS = 11
PLACE = {8: list(range(8)), 4: [0, 1, 2, 7], 2: [0, 7]}
MESH = pl.DeviceIdType.MESH
HIGHEST = lax.Precision.HIGHEST
AREA = [(dx, dy) for dx in (-1, 0, 1) for dy in (-1, 0, 1)]
FLAT = [d for d in AREA if d != (0, 0)]


def legendre_pair(point, degree):
    previous = 1.0
    current = point
    for order in range(1, degree):
        following = ((2 * order + 1) * point * current - order * previous) / (order + 1)
        previous = current
        current = following
    return (current, previous)


def gll_tables(points):
    degree = points - 1
    node_list = []
    for index in range(points):
        guess = -math.cos(math.pi * index / degree)
        for sweep in range(100):
            high_val, low_val = legendre_pair(guess, degree)
            guess = guess - (guess * high_val - low_val) / (points * high_val)
        node_list.append(guess)
    node_list[0] = -1.0
    node_list[degree] = 1.0
    node_pos = np.array(node_list)
    at_nodes = np.array([legendre_pair(value, degree)[0] for value in node_list])
    weights = 2.0 / (degree * (degree + 1) * at_nodes**2)
    derivative = np.zeros((points, points))
    for row_pos in range(points):
        for col_pos in range(points):
            if row_pos != col_pos:
                derivative[row_pos, col_pos] = at_nodes[row_pos] / (
                    at_nodes[col_pos] * (node_pos[row_pos] - node_pos[col_pos])
                )
    derivative[0, 0] = -degree * (degree + 1) / 4.0
    derivative[degree, degree] = degree * (degree + 1) / 4.0
    stiffness = derivative.T @ (weights[:, None] * derivative)
    return (node_pos, weights, stiffness)


def interp_table(fine_pts, coarse_pts):
    fine_nodes = gll_tables(fine_pts)[0]
    coarse_nodes = gll_tables(coarse_pts)[0]
    lagrange = np.ones((fine_pts, coarse_pts))
    for col_pos in range(coarse_pts):
        for other_pos in range(coarse_pts):
            if other_pos != col_pos:
                lagrange[:, col_pos] *= (fine_nodes - coarse_nodes[other_pos]) / (
                    coarse_nodes[col_pos] - coarse_nodes[other_pos]
                )
    return lagrange


def constant_tables():
    parts = {}
    same = np.eye(NE)
    for points in (NF, NM):
        at = PLACE[points]
        _, short_w, short_k = gll_tables(points)
        short_w = short_w.astype(np.float32).astype(np.float64)
        short_k = short_k.astype(np.float32).astype(np.float64)
        w = np.zeros(8)
        w[at] = short_w
        k = np.zeros((8, 8))
        k[np.ix_(at, at)] = short_k
        kd = np.diag(k)
        parts["left%d" % points] = np.concatenate([np.kron(k, np.diag(w)), np.kron(np.diag(w), k)])
        parts["right%d" % points] = np.kron(same, k.T)
        parts["wab%d" % points] = np.repeat(np.kron(w, w)[:, None], LANES, 1)
        lane_w, lane_k = np.tile(w, NE), np.tile(kd, NE)
        parts["dx%d" % points] = np.kron(kd, w)[:, None] * lane_w
        parts["dy%d" % points] = np.kron(w, kd)[:, None] * lane_w
        parts["dz%d" % points] = np.kron(w, w)[:, None] * lane_k
        parts["lane%d" % points] = np.repeat(lane_w[None], 8, 0)
    for fine, coarse, name in ((NF, NM, "f"), (NM, NC, "c")):
        j = np.zeros((8, 8))
        j[np.ix_(PLACE[fine], PLACE[coarse])] = interp_table(fine, coarse)
        parts["down_left_" + name] = np.kron(j, j).T
        parts["down_right_" + name] = np.kron(same, j)
        parts["up_left_" + name] = np.kron(j, j)
        parts["up_right_" + name] = np.kron(same, j.T)
    parts["spread"] = np.kron(same, np.ones((1, 8)))
    ends = ((0, 64), (64, 0), (63, 127), (127, 63))
    pick = np.zeros((32, LANES))
    for index, pair in enumerate(ends):
        for row, lane in enumerate(pair):
            pick[index * 8 + row, lane] = 1.0
    parts["pick"] = pick
    put = np.zeros((8, LANES))
    for row, lane in enumerate((0, 64, 63, 127)):
        put[row, lane] = 1.0
    parts["put"] = put
    own_low, own_top = np.zeros((24, LANES)), np.zeros((24, LANES))
    for z in range(8):
        own_low[z, z * 8] = 1.0
        own_low[8 + z, 64 + z * 8] = 1.0
        own_top[16 + z, 64 + z * 8] = 1.0
    parts["own_low"], parts["own_top"] = own_low, own_top
    start, rows, where = 0, [], {}
    for name, part in parts.items():
        where[name] = (start, part.shape[0], part.shape[1])
        start += part.shape[0]
        rows.append(np.pad(part, ((0, 0), (0, LANES - part.shape[1]))))
    return np.concatenate(rows).astype(np.float32), where


def dot(a, b):
    return jnp.dot(a, b, precision=HIGHEST, preferred_element_type=jnp.float32)


def split(value):
    high = value.astype(jnp.bfloat16)
    return high, (value - high.astype(jnp.float32)).astype(jnp.bfloat16)


def dot3(a, b):
    (a_high, a_low), (b_high, b_low) = split(a), split(b)

    def one(left, right):
        return jnp.dot(left, right, preferred_element_type=jnp.float32)

    return one(a_high, b_high) + (one(a_high, b_low) + one(a_low, b_high))


def dot_nt(a, b):
    return lax.dot_general(
        a, b, (((1,), (1,)), ((), ())), precision=HIGHEST, preferred_element_type=jnp.float32
    )


def dot_tn(a, b):
    return lax.dot_general(
        a, b, (((0,), (0,)), ((), ())), precision=HIGHEST, preferred_element_type=jnp.float32
    )


def kernel(
    sizes, where, src_far, geo_ref, eig_ref, rows_far, ids_ref, tab_far, out_ref,
    src_ref, rows_ref, tab_ref, near_sems, work, ysend, zsend, xyrecv, zrecv, zin, idsend, idrecv, csend, crecv, colsend, rsrecv,
    zpsend, zprecv, agsend, agrecv, backsend, backrecv,
    xy_sems, z_sems, id_sems, c_sems, rs_sems, zp_sems, ag_sems, back_sems,
):
    n_x, n_y, n_z = sizes
    fetch_tab = pltpu.make_async_copy(tab_far, tab_ref, near_sems.at[0])
    fetch_rows = pltpu.make_async_copy(rows_far, rows_ref, near_sems.at[1])
    fetch_src = pltpu.make_async_copy(src_far, src_ref, near_sems.at[2])
    fetch_src.start()
    fetch_tab.start()
    fetch_rows.start()
    crecv[...] = jnp.zeros_like(crecv)
    me_x, me_y, me_z = lax.axis_index("gx"), lax.axis_index("gy"), lax.axis_index("gz")
    bx, by, bz = n_x // 2, n_y // 4, n_z // 2
    my_place = (me_x % 2) * 8 + (me_y % 4) * 2 + me_z % 2
    my_block = (me_x // 2) * by + me_y // 4

    def table(name):
        start, count, width = where[name]
        return tab_ref[pl.ds(start, count), pl.ds(0, width)]

    def near(dx, dy, dz):
        return ((me_x + dx + n_x) % n_x, (me_y + dy + n_y) % n_y, (me_z + dz + n_z) % n_z)

    def mate(ux, uy, uz):
        px, py, pz = (me_x % 2 + ux) % 2, (me_y % 4 + uy) % 4, (me_z % 2 + uz) % 2
        who = ((me_x // 2) * 2 + px, (me_y // 4) * 4 + py, (me_z // 2) * 2 + pz)
        return who, px * 8 + py * 2 + pz

    def across(tx, ty):
        qx, qy = (me_x // 2 + tx) % bx, (me_y // 4 + ty) % by
        return (qx * 2 + me_x % 2, qy * 4 + me_y % 4, me_z), qx * by + qy

    def along(tz):
        return (me_x, me_y, ((me_z // 2 + tz) % bz) * 2 + me_z % 2)

    mates = [mate(i // 8, i // 2 % 4, i % 2) for i in range(1, 16)]
    crosses = [across(i // by, i % by) for i in range(1, bx * by)]
    lines = [along(i) for i in range(1, bz)]

    barrier = pltpu.get_barrier_semaphore()
    peers = [near(dx, dy, dz) for dx, dy in AREA for dz in (-1, 0, 1) if (dx, dy, dz) != (0, 0, 0)]
    peers += [who for who, _ in mates] + [who for who, _ in crosses] + lines
    for who in peers:
        pl.semaphore_signal(barrier, inc=1, device_id=who, device_id_type=MESH)

    def send(src, dst, sems, who):
        pltpu.make_async_remote_copy(
            src_ref=src, dst_ref=dst, send_sem=sems.at[0], recv_sem=sems.at[1],
            device_id=who, device_id_type=MESH,
        ).start()

    def await_all(ref, sems):
        every = pltpu.make_async_remote_copy(
            src_ref=ref, dst_ref=ref, send_sem=sems.at[0], recv_sem=sems.at[1],
            device_id=near(1, 0, 0), device_id_type=MESH,
        )
        every.wait_recv()
        every.wait_send()

    lane = lax.broadcasted_iota(jnp.int32, (8, LANES), 1)
    row = lax.broadcasted_iota(jnp.int32, (8, LANES), 0)
    low_half = lane < 64
    row64 = lax.broadcasted_iota(jnp.int32, (ROWS, LANES), 0)
    lane64 = lax.broadcasted_iota(jnp.int32, (ROWS, LANES), 1)
    node, elem = lane64 % 8, lane64 // 8 % 8
    join_up = (node == 7) & (elem < 7)
    join_down = (node == 0) & (elem > 0)
    edge_y = ((row64 % 8 == 0) & (lane64 < 64)) | ((row64 % 8 == 7) & (lane64 >= 64))
    has_low = (me_y > 0).astype(jnp.float32)
    has_high = (me_y < n_y - 1).astype(jnp.float32)
    at_top = (me_y == n_y - 1).astype(jnp.float32)

    def roll(value, shift, axis):
        return pltpu.roll(value, shift % value.shape[axis], axis)

    def sum_pack(slot, value):
        field = work.at[slot]
        value = (
            value
            + jnp.where(join_up, roll(value, -1, 1), 0.0)
            + jnp.where(join_down, roll(value, 1, 1), 0.0)
        )
        field[pl.ds(0, ROWS), :] = value
        low = field[pl.ds(0, 8, stride=8), :]
        high = field[pl.ds(7, 8, stride=8), :]
        new_low = low + jnp.where(low_half, 0.0, roll(high, 64, 1))
        new_high = high + jnp.where(low_half, roll(low, 64, 1), 0.0)
        field[pl.ds(0, 8, stride=8), :] = new_low
        field[pl.ds(7, 8, stride=8), :] = new_high
        ysend[slot] = jnp.where(low_half, new_low, new_high)
        ends = dot_nt(table("pick"), field[...])
        for index, (dx, dy) in enumerate(AREA):
            keep = low_half
            if dx:
                keep = keep & (lane // 8 == (0 if dx > 0 else 7))
            if dy:
                keep = keep & (lane % 8 == (0 if dy > 0 else 7)) & (row == (0 if dy > 0 else 1))
            for side in (0, 1):
                variant = 2 * side + (1 if dy else 0)
                tile = ends[variant * 8 : variant * 8 + 8]
                moved = jnp.where(keep, roll(tile, -56 * dx - 7 * dy, 1), 0.0)
                zsend[slot, index * 2 + side] = moved[0:2]

    def sum_send(slot, fields=1):
        span = pl.ds(slot, fields)
        order = [(dx, dy, dz) for dx, dy in AREA for dz in (-1, 0, 1) if (dx, dy, dz) != (0, 0, 0)]
        for dx, dy, dz in sorted(order, key=lambda d: -sum(map(abs, d))):
            if dz:
                side = 0 if dz < 0 else 1
                src = zsend.at[span, AREA.index((dx, dy)) * 2 + side]
                dst = zrecv.at[span, AREA.index((-dx, -dy)) * 2 + side]
                send(src, dst, z_sems.at[slot], near(dx, dy, dz))
            else:
                if dy:
                    src = ysend.at[span]
                else:
                    src = work.at[span, pl.ds(56 if dx > 0 else 0, 8), :]
                dst = xyrecv.at[span, FLAT.index((-dx, -dy))]
                send(src, dst, xy_sems.at[slot], near(dx, dy, dz))

    def sum_await(slot, fields=1):
        await_all(xyrecv.at[pl.ds(slot, fields)], xy_sems.at[slot])
        await_all(zrecv.at[pl.ds(slot, fields)], z_sems.at[slot])

    def sum_finish(slot):
        tiles = {d: xyrecv[slot, i] for i, d in enumerate(FLAT)}

        def edge(dy):
            return (
                tiles[(0, dy)]
                + jnp.where(row == 7, roll(tiles[(1, dy)], 7, 0), 0.0)
                + jnp.where(row == 0, roll(tiles[(-1, dy)], 1, 0), 0.0)
            )

        from_y = roll(jnp.where(low_half, edge(1) * has_high, edge(-1) * has_low), 64, 1)
        value = work[slot, pl.ds(0, ROWS), :]
        spread = jnp.broadcast_to(from_y[:, None, :], (8, 8, LANES)).reshape(ROWS, LANES)
        value = value + jnp.where(edge_y, spread, 0.0)
        value = value + jnp.concatenate(
            [tiles[(-1, 0)], jnp.zeros((48, LANES), jnp.float32), tiles[(1, 0)]], axis=0
        )
        for side in (0, 1):
            parts = []
            for dy in (-1, 0, 1):
                part = sum(zrecv[slot, AREA.index((dx, dy)) * 2 + side] for dx in (-1, 0, 1))
                parts.append(part if dy == 0 else part * (has_low if dy < 0 else has_high))
            target = 2 * (1 - side)
            zin[pl.ds(target, 2), :] = parts[0] + parts[1] + parts[2]
        return value + dot_tn(zin[...], table("put"))[0:ROWS]

    turn = [OPENING]

    def direct_sum(value):
        slot = turn[0] % SLOTS
        turn[0] += 1
        sum_pack(slot, value)
        sum_send(slot)
        sum_await(slot)
        return sum_finish(slot)

    fetch_src.wait()
    fetch_tab.wait()
    for slot in range(SLOTS):
        work[slot, pl.ds(ROWS, ROWS), :] = jnp.zeros((ROWS, LANES), jnp.float32)
    zin[...] = jnp.zeros_like(zin)

    geo = dot(geo_ref[:, 0, :], table("spread")[0:8]) + dot(geo_ref[:, 1, :], table("spread")[8:16])
    geo = [geo[i : i + 1] for i in range(3)]

    spread16 = dot_tn(src_ref[...], table("spread"))
    deep_row = lax.broadcasted_iota(jnp.int32, (NE * 32, LANES), 0)
    deep_lane = lax.broadcasted_iota(jnp.int32, (NE * 32, LANES), 1)
    same_node = deep_row % 8 == deep_lane % 8
    source = jnp.sum(jnp.where(same_node, spread16, 0.0).reshape(ROWS, 8, LANES), axis=1)

    def diagonal(points):
        return sum(g * table("d%s%d" % (axis, points)) for g, axis in zip(geo, "xyz"))

    scaled = {}
    for points in (NF, NM):
        lane_w = table("lane%d" % points)[0:1]
        scaled[points] = (geo[0] * lane_w, geo[1] * lane_w, geo[2] * table("wab%d" % points))

    def local_apply(value, points):
        in_x, in_y, in_z = scaled[points]
        both = dot3(table("left%d" % points), value)
        return (
            in_x * both[0:ROWS]
            + in_y * both[ROWS : 2 * ROWS]
            + in_z * dot3(value, table("right%d" % points))
        )

    def move(value, way):
        left, right = way.split("-")
        return dot3(dot3(table(left), value), table(right))

    def cheb_numbers(index):
        lam = jnp.full((1, LANES), eig_ref[index], jnp.float32)
        center = 0.55 * lam
        spread_eig = 0.45 * lam
        ratio = center / spread_eig
        first = 1.0 / ratio
        following = 1.0 / (2.0 * ratio - first)
        return 1.0 / center, first * following, 2.0 * following / spread_eig

    small_lane = lax.broadcasted_iota(jnp.int32, (2, LANES), 1)
    small_row = lax.broadcasted_iota(jnp.int32, (2, LANES), 0)
    spot = small_row * LANES + small_lane - my_place * 16
    own_ids = jnp.zeros((2, LANES), jnp.float32)
    for k in range(BLOCKS):
        number = jnp.full((2, LANES), ids_ref[k], jnp.int32).astype(jnp.float32) + 1.0
        own_ids = jnp.where(spot == k, number, own_ids)
    idsend[...] = own_ids

    sum_pack(0, source)
    sum_pack(1, diagonal(NF))
    sum_pack(2, diagonal(NM))
    pl.semaphore_wait(barrier, len(peers))
    sum_send(0, OPENING)
    for i, (who, _) in enumerate(mates):
        send(idsend, idrecv.at[i], id_sems, who)
    sum_await(0, OPENING)
    fine_res = sum_finish(0)
    fine_inv = 1.0 / sum_finish(1)
    mid_diag = sum_finish(2)
    mid_inv = jnp.where(mid_diag > 0.0, 1.0 / jnp.where(mid_diag > 0.0, mid_diag, 1.0), 0.0)

    def chebyshev(residual, initial, numbers, points, inverse):
        by_center, first, second = numbers
        if initial is None:
            current = residual
        else:
            current = residual - direct_sum(local_apply(initial, points))
        step_one = inverse * current * by_center
        iterate = step_one if initial is None else initial + step_one
        left = residual - direct_sum(local_apply(iterate, points))
        return iterate + (first * step_one + second * (inverse * left))

    fine_numbers, mid_numbers = cheb_numbers(0), cheb_numbers(1)
    fine_x = chebyshev(fine_res, None, fine_numbers, NF, fine_inv)
    mid_src = move(source - local_apply(fine_x, NF), "down_left_f-down_right_f")
    mid_res = direct_sum(mid_src)
    mid_x = chebyshev(mid_res, None, mid_numbers, NM, mid_inv)
    low_res = direct_sum(move(mid_src - local_apply(mid_x, NM), "down_left_c-down_right_c"))

    own_low = table("own_low")
    own_top = table("own_top") * at_top
    owned = jnp.sum(own_low * low_res[0:1] + own_top * low_res[7:8], axis=1, keepdims=True)
    owned = jnp.broadcast_to(owned, (24, LANES)).reshape(3, 8, LANES)
    fetch_rows.wait()
    contrib = (
        owned[0:1] * rows_ref[0] + owned[1:2] * rows_ref[1] + owned[2:3] * rows_ref[2]
    )
    contrib = jnp.sum(contrib, axis=1)
    csend[...] = contrib
    for who, _ in mates:
        send(csend, crecv.at[my_place, pl.ds(0, BLOCKS)], c_sems, who)
    crecv[my_place, pl.ds(0, BLOCKS)] = contrib

    await_all(idrecv, id_sems)
    all_ids = own_ids
    for i in range(15):
        all_ids = all_ids + idrecv[i]
    wanted = (
        lax.broadcasted_iota(jnp.int32, (LANES, LANES), 0) + my_place * LANES + 1
    ).astype(jnp.float32)
    match_a = (all_ids[0:1] == wanted).astype(jnp.float32)
    match_b = (all_ids[1:2] == wanted).astype(jnp.float32)

    await_all(crecv.at[pl.ds(0, 15), pl.ds(0, BLOCKS)], c_sems)
    part = dot(match_a, crecv[pl.ds(0, 8)].reshape(LANES, LANES)) + dot(
        match_b, crecv[pl.ds(8, 8)].reshape(LANES, LANES)
    )
    peers_xy = bx * by
    height = LANES // peers_xy
    colsend[...] = part.reshape(peers_xy, height, LANES)
    for i, (who, block) in enumerate(crosses):
        send(colsend.at[block], rsrecv.at[i], rs_sems, who)
    piece = colsend[my_block]
    await_all(rsrecv, rs_sems)
    for i in range(peers_xy - 1):
        piece = piece + rsrecv[i]
    zpsend[...] = piece
    for i, who in enumerate(lines):
        send(zpsend, zprecv.at[i], zp_sems, who)
    await_all(zprecv, zp_sems)
    for i in range(bz - 1):
        piece = piece + zprecv[i]
    agsend[...] = piece
    for who, _ in crosses:
        send(agsend, agrecv.at[my_block], ag_sems, who)
    agrecv[my_block] = piece
    await_all(agrecv.at[pl.ds(0, peers_xy - 1)], ag_sems)
    slice_sum = agrecv[...].reshape(LANES, LANES)
    backsend[pl.ds(0, 8)] = dot_tn(match_a, slice_sum).reshape(8, 16, LANES)
    backsend[pl.ds(8, 8)] = dot_tn(match_b, slice_sum).reshape(8, 16, LANES)
    for i, (who, place) in enumerate(mates):
        send(backsend.at[place, pl.ds(0, BLOCKS)], backrecv.at[i], back_sems, who)
    picked = backsend[my_place, pl.ds(0, BLOCKS)]
    await_all(backrecv, back_sems)
    for i in range(15):
        picked = picked + backrecv[i]

    solved = jnp.concatenate(
        [sum(rows_ref[j, k] * picked[k : k + 1] for k in range(BLOCKS)) for j in range(3)], axis=0
    )
    solved = jnp.sum(solved, axis=1, keepdims=True)
    at_low = jnp.sum(own_low * solved, axis=0, keepdims=True)
    at_high = jnp.sum(own_top * solved, axis=0, keepdims=True)
    low_u = direct_sum(
        jnp.where(row64 == 0, at_low, 0.0) + jnp.where(row64 == 7, at_high, 0.0)
    )
    mid_x = chebyshev(mid_res, mid_x + move(low_u, "up_left_c-up_right_c"), mid_numbers, NM, mid_inv)
    fine_x = chebyshev(
        fine_res, fine_x + move(mid_x, "up_left_f-up_right_f"), fine_numbers, NF, fine_inv
    )
    deep = jnp.broadcast_to(fine_x[:, None, :], (ROWS, 8, LANES)).reshape(ROWS * 8, LANES)
    out_ref[...] = dot_nt(table("spread"), jnp.where(same_node, deep, 0.0))


def solution(mesh):
    sizes = (mesh.shape["gx"], mesh.shape["gy"], mesh.shape["gz"])
    values, where = constant_tables()
    peers_xy = (sizes[0] // 2) * (sizes[1] // 4)
    height = LANES // peers_xy
    depth = sizes[2] // 2
    f32 = jnp.float32

    def on_device(residual_in, geometry, eig_top, coarse_rows, block_ids):
        vmem = pl.BlockSpec(memory_space=pltpu.VMEM)
        smem = pl.BlockSpec(memory_space=pltpu.SMEM)
        far = pl.BlockSpec(memory_space=pltpu.HBM)
        pair = pltpu.SemaphoreType.DMA((2,))
        out = pl.pallas_call(
            functools.partial(kernel, sizes, where),
            out_shape=jax.ShapeDtypeStruct((NE, NF**3), f32),
            in_specs=[far, vmem, smem, far, smem, far],
            out_specs=vmem,
            scratch_shapes=[
                pltpu.VMEM((NE, NF**3), f32),
                pltpu.VMEM((3, BLOCKS, 8, LANES), f32),
                pltpu.VMEM(values.shape, f32),
                pltpu.SemaphoreType.DMA((3,)),
                pltpu.VMEM((SLOTS, 2 * ROWS, LANES), f32),
                pltpu.VMEM((SLOTS, 8, LANES), f32),
                pltpu.VMEM((SLOTS, 18, 2, LANES), f32),
                pltpu.VMEM((SLOTS, 8, 8, LANES), f32),
                pltpu.VMEM((SLOTS, 18, 2, LANES), f32),
                pltpu.VMEM((8, LANES), f32),
                pltpu.VMEM((2, LANES), f32),
                pltpu.VMEM((15, 2, LANES), f32),
                pltpu.VMEM((BLOCKS, LANES), f32),
                pltpu.VMEM((16, 16, LANES), f32),
                pltpu.VMEM((peers_xy, height, LANES), f32),
                pltpu.VMEM((peers_xy - 1, height, LANES), f32),
                pltpu.VMEM((height, LANES), f32),
                pltpu.VMEM((depth - 1, height, LANES), f32),
                pltpu.VMEM((height, LANES), f32),
                pltpu.VMEM((peers_xy, height, LANES), f32),
                pltpu.VMEM((16, 16, LANES), f32),
                pltpu.VMEM((15, BLOCKS, LANES), f32),
                pltpu.SemaphoreType.DMA((SLOTS, 2)),
                pltpu.SemaphoreType.DMA((SLOTS, 2)),
                pair, pair, pair, pair, pair, pair,
            ],
            compiler_params=pltpu.CompilerParams(
                collective_id=0, has_side_effects=True, vmem_limit_bytes=56500000
            ),
        )(
            residual_in.reshape(NE, NF**3),
            geometry.reshape(3, 2, 8),
            eig_top,
            jnp.swapaxes(coarse_rows.reshape(3, 8, BLOCKS, LANES), 1, 2),
            block_ids.reshape(BLOCKS),
            jnp.asarray(values),
        )
        return out.reshape(residual_in.shape)

    grid = P("gx", "gy", "gz", None)
    return jax.shard_map(
        on_device,
        mesh=mesh,
        in_specs=(grid, P(None, "gx", "gy", "gz"), P(), P("gx", "gy", "gz", None, None), grid),
        out_specs=grid,
        check_vma=False,
    )
```
